32 devices in a mesh: lat: 2 (over x), lon: 4 (over y, core), lev: 4 (over z).
Axes of the slice: x: 2, y: 2, z: 4, core: 2. Of those that a mesh axis runs over, the one named last changes fastest.
Arguments:
- initial_state: float32 [8, 384, 128, 128], P('lat', 'lon', 'lev'), may hold values from 0.5 to 2
- scaled_wind_north: float32 [8, 384, 128, 128], P('lat', 'lon', 'lev'), may hold values from -0.3 to 0.3
- scaled_wind_east: float32 [8, 384, 128, 128], P('lat', 'lon', 'lev'), may hold values from -0.3 to 0.3
- scaled_wind_upward: float32 [8, 384, 128, 128], P('lat', 'lon', 'lev'), may hold values from -0.3 to 0.3
Outputs:
- normalised_state: float32 [8, 384, 128, 128], P('lat', 'lon', 'lev')
- temperature_end: float32 [8, 384, 128, 128], P('lat', 'lon', 'lev')
The draws below stay inside these ranges and needn't reach their ends.
All inputs are finite; a program needn't handle non-finite values.
Results may differ from the reference program's by a relative error of at most 0.00002.
Values sent between devices are 32-bit elements; how exact they have to be, the bound alone decides.
A program may use at most 128 MiB of HBM per device.

```python
import jax
import jax.numpy as jnp
from jax import lax

CELLS_NORTHWARD = 8
CELLS_EASTWARD = 384
CELLS_UPWARD = 128
MEMBER_TOTAL = 128
STEPS = 4


def block_scale(rng, extent, pieces, low, high):
    def one(position, blocks):
        steps = jax.random.uniform(jax.random.fold_in(jax.random.fold_in(rng, 6), position), (blocks,), jnp.float32, low / len(pieces), high / len(pieces))
        return jnp.repeat(jnp.exp(steps), extent[position] // blocks).reshape((-1,) + (1,) * (len(extent) - position - 1))

    gain = one(*pieces[0])
    for cut in pieces[1:]:
        gain = gain * one(*cut)
    return gain


def setup_inputs(seed: int = 0) -> dict:
    key_of = jax.random.split(jax.random.key(seed), 5)
    return {
        "initial_state": jnp.clip(0.5 + 1.5 * jax.random.uniform(key_of[0], (CELLS_NORTHWARD, CELLS_EASTWARD, CELLS_UPWARD, MEMBER_TOTAL), jnp.float32) ** block_scale(key_of[0], (CELLS_NORTHWARD, CELLS_EASTWARD, CELLS_UPWARD, MEMBER_TOTAL), ((0, 2), (1, 4), (2, 4)), -0.2, 0.2), 0.5, 2.0),
        "scaled_wind_north": jnp.clip(jax.random.uniform(key_of[1], (CELLS_NORTHWARD, CELLS_EASTWARD, CELLS_UPWARD, MEMBER_TOTAL), jnp.float32, -0.3, 0.3) * block_scale(key_of[1], (CELLS_NORTHWARD, CELLS_EASTWARD, CELLS_UPWARD, MEMBER_TOTAL), ((0, 2), (1, 4), (2, 4)), -0.4, 0.0), -0.3, 0.3),
        "scaled_wind_east": jnp.clip(jax.random.uniform(key_of[2], (CELLS_NORTHWARD, CELLS_EASTWARD, CELLS_UPWARD, MEMBER_TOTAL), jnp.float32, -0.3, 0.3) * block_scale(key_of[2], (CELLS_NORTHWARD, CELLS_EASTWARD, CELLS_UPWARD, MEMBER_TOTAL), ((0, 2), (1, 4), (2, 4)), -0.4, 0.0), -0.3, 0.3),
        "scaled_wind_upward": jnp.clip(jax.random.uniform(key_of[3], (CELLS_NORTHWARD, CELLS_EASTWARD, CELLS_UPWARD, MEMBER_TOTAL), jnp.float32, -0.3, 0.3) * block_scale(key_of[3], (CELLS_NORTHWARD, CELLS_EASTWARD, CELLS_UPWARD, MEMBER_TOTAL), ((0, 2), (1, 4), (2, 4)), -0.4, 0.0), -0.3, 0.3),
    }


def strip_edges(values, dims):
    for dim in dims:
        values = lax.slice_in_dim(values, 1, values.shape[dim] - 1, axis=dim)
    return values

def neighbour(values, dim, start, dims):
    others = [other for other in dims if other != dim]
    values = strip_edges(values, others)
    return lax.slice_in_dim(values, start, start + values.shape[dim] - 2, axis=dim)

def march_one_step(padded_state, scaled_wind_north, scaled_wind_east, scaled_wind_upward):
    middle = strip_edges(padded_state, (0, 1, 2))
    lower = [neighbour(padded_state, dim, 0, (0, 1, 2)) for dim in (0, 1, 2)]
    upper = [neighbour(padded_state, dim, 2, (0, 1, 2)) for dim in (0, 1, 2)]
    slopes = [above - below for above, below in zip(upper, lower)]
    smooth_rate = 0.05
    spread = lower[0] + upper[0] + lower[1] + upper[1] + lower[2] + upper[2] - 6.0 * middle
    return middle - scaled_wind_north * slopes[0] - scaled_wind_east * slopes[1] - scaled_wind_upward * slopes[2] + smooth_rate * spread

def reference(initial_state, scaled_wind_north, scaled_wind_east, scaled_wind_upward):
    for step in range(STEPS):
        initial_state = march_one_step(jnp.pad(initial_state, ((1, 1), (1, 1), (1, 1), (0, 0)), mode='constant'), scaled_wind_north, scaled_wind_east, scaled_wind_upward)
    vertical_mean = lax.optimization_barrier(jnp.mean(initial_state, axis=1, keepdims=True))
    symmetric_slope = initial_state - vertical_mean
    line_variance = lax.optimization_barrier(jnp.mean(symmetric_slope * symmetric_slope, axis=1, keepdims=True))
    normalised_state = symmetric_slope * lax.rsqrt(line_variance + 0.0001)
    return (normalised_state, initial_state)
```

```python
import functools

import jax
import jax.numpy as jnp
from jax import lax
from jax.experimental import pallas as pl
from jax.experimental.pallas import tpu as pltpu
from jax.sharding import PartitionSpec as P

STEPS = 4
RATE = 0.05
EPS = 0.0001
MESH = pl.DeviceIdType.MESH
MIB = 1024 * 1024


def pieces_of(cells):
    return max(d for d in range(1, 9) if cells % d == 0)


def march_kernel(
    pieces, state_hbm, north_hbm, east_hbm, up_hbm, out_ref, stat_ref,
    cells, winds, lev_out, lev_in, stat_in,
    load_sem, lat_send, lat_recv, lon_send, lon_recv, lev_send, lev_recv, stat_send, stat_recv,
):
    rows, width, depth, members = out_ref.shape
    piece = width // pieces
    lat, lon, lev = lax.axis_index("lat"), lax.axis_index("lon"), lax.axis_index("lev")
    lats, lons, levs = lax.axis_size("lat"), lax.axis_size("lon"), lax.axis_size("lev")
    has_lat = (lat > 0, lat < lats - 1)
    has_lon = (lon > 0, lon < lons - 1)
    has_lev = (lev > 0, lev < levs - 1)
    lat_peer = (jnp.maximum(lat - 1, 0), jnp.minimum(lat + 1, lats - 1))
    lon_peer = (jnp.maximum(lon - 1, 0), jnp.minimum(lon + 1, lons - 1))
    lev_peer = (jnp.maximum(lev - 1, 0), jnp.minimum(lev + 1, levs - 1))

    loads = [
        pltpu.make_async_copy(
            state_hbm, cells.at[0, pl.ds(1, rows), pl.ds(1, width)], load_sem.at[0]
        )
    ]
    for k, ref in enumerate((north_hbm, east_hbm, up_hbm)):
        loads.append(pltpu.make_async_copy(ref, winds.at[k], load_sem.at[k + 1]))
    for load in loads:
        load.start()

    barrier = pltpu.get_barrier_semaphore()
    arrivals = lons - 1
    for axis, has, peer in (("lat", has_lat, lat_peer), ("lev", has_lev, lev_peer)):
        for side in (0, 1):
            arrivals = arrivals + has[side].astype(jnp.int32)

            @pl.when(has[side])
            def _(axis=axis, target=peer[side]):
                pl.semaphore_signal(barrier, inc=1, device_id={axis: target}, device_id_type=MESH)

    for k in range(1, lons):
        pl.semaphore_signal(
            barrier, inc=1, device_id={"lon": lax.rem(lon + k, lons)}, device_id_type=MESH
        )
    pl.semaphore_wait(barrier, arrivals)

    def lat_copy(parity, side, c, from_hbm=False):
        span = pl.ds(c * piece, piece)
        padded = pl.ds(1 + c * piece, piece)
        row = 0 if side == 0 else rows - 1
        src = state_hbm.at[row, span] if from_hbm else cells.at[parity, row + 1, padded]
        return pltpu.make_async_remote_copy(
            src_ref=src,
            dst_ref=cells.at[parity, rows + 1 if side == 0 else 0, padded],
            send_sem=lat_send.at[parity, side, c],
            recv_sem=lat_recv.at[parity, 1 - side, c],
            device_id={"lat": lat_peer[side]},
            device_id_type=MESH,
        )

    def lat_arrival(parity, side, c):
        here = cells.at[parity, 0 if side == 0 else rows + 1, pl.ds(1 + c * piece, piece)]
        return pltpu.make_async_remote_copy(
            src_ref=here, dst_ref=here,
            send_sem=lat_send.at[parity, side, c], recv_sem=lat_recv.at[parity, side, c],
            device_id={"lat": lat_peer[side]}, device_id_type=MESH,
        )

    def lon_copy(parity, side, from_hbm=False):
        col = 0 if side == 0 else width - 1
        mine = pl.ds(1, rows)
        src = state_hbm.at[:, col] if from_hbm else cells.at[parity, mine, col + 1]
        return pltpu.make_async_remote_copy(
            src_ref=src,
            dst_ref=cells.at[parity, mine, width + 1 if side == 0 else 0],
            send_sem=lon_send.at[parity, side],
            recv_sem=lon_recv.at[parity, 1 - side],
            device_id={"lon": lon_peer[side]},
            device_id_type=MESH,
        )

    def lon_arrival(parity, side):
        here = cells.at[parity, pl.ds(1, rows), 0 if side == 0 else width + 1]
        return pltpu.make_async_remote_copy(
            src_ref=here, dst_ref=here,
            send_sem=lon_send.at[parity, side], recv_sem=lon_recv.at[parity, side],
            device_id={"lon": lon_peer[side]}, device_id_type=MESH,
        )

    def lev_copy(parity, side):
        return pltpu.make_async_remote_copy(
            src_ref=lev_out.at[parity, side],
            dst_ref=lev_in.at[parity, 1 - side],
            send_sem=lev_send.at[parity, side],
            recv_sem=lev_recv.at[parity, 1 - side],
            device_id={"lev": lev_peer[side]},
            device_id_type=MESH,
        )

    def lev_arrival(parity, side):
        here = lev_in.at[parity, side]
        return pltpu.make_async_remote_copy(
            src_ref=here, dst_ref=here,
            send_sem=lev_send.at[parity, side], recv_sem=lev_recv.at[parity, side],
            device_id={"lev": lev_peer[side]}, device_id_type=MESH,
        )

    def each_side(has, act):
        for side in (0, 1):
            @pl.when(has[side])
            def _(side=side):
                act(side)

    def first_sends(c, carry):
        each_side(has_lat, lambda side: lat_copy(0, side, c, True).start())
        return carry

    lax.fori_loop(0, pieces, first_sends, 0)
    each_side(has_lon, lambda side: lon_copy(0, side, True).start())

    for side in (0, 1):
        @pl.when(jnp.logical_not(has_lat[side]))
        def _(row=0 if side == 0 else rows + 1):
            def clear(x, carry):
                for parity in (0, 1):
                    cells[parity, row, x + 1] = jnp.zeros((depth, members), jnp.float32)
                return carry

            lax.fori_loop(0, width, clear, 0)

        @pl.when(jnp.logical_not(has_lon[side]))
        def _(col=0 if side == 0 else width + 1):
            for parity in (0, 1):
                for y in range(rows):
                    cells[parity, y + 1, col] = jnp.zeros((depth, members), jnp.float32)

        @pl.when(jnp.logical_not(has_lev[side]))
        def _(side=side):
            def clear(x, carry):
                for parity in (0, 1):
                    for y in range(rows):
                        lev_in[parity, side, y, x] = jnp.zeros((1, members), jnp.float32)
                return carry

            lax.fori_loop(0, width, clear, 0)

    loads[0].wait()

    def first_levels(x, carry):
        for y in range(rows):
            lev_out[0, 0, y, x] = cells[0, y + 1, x + 1, 0:1, :]
            lev_out[0, 1, y, x] = cells[0, y + 1, x + 1, depth - 1 : depth, :]
        return carry

    lax.fori_loop(0, width, first_levels, 0)
    each_side(has_lev, lambda side: lev_copy(0, side).start())
    for load in loads[1:]:
        load.wait()

    level = lax.broadcasted_iota(jnp.int32, (depth, members), 0)
    bottom, top = level == 0, level == depth - 1

    def advance(parity, y, x):
        mid = cells[parity, y + 1, x + 1]
        south, north = cells[parity, y, x + 1], cells[parity, y + 2, x + 1]
        west, east = cells[parity, y + 1, x], cells[parity, y + 1, x + 2]
        below = jnp.where(bottom, lev_in[parity, 0, y, x], pltpu.roll(mid, 1, 0))
        above = jnp.where(top, lev_in[parity, 1, y, x], pltpu.roll(mid, depth - 1, 0))
        spread = (south + north) + (west + east) + (below + above) - 6.0 * mid
        return (
            mid
            - winds[0, y, x] * (north - south)
            - winds[1, y, x] * (east - west)
            - winds[2, y, x] * (above - below)
            + RATE * spread
        )

    for t in range(STEPS - 1):
        now, later = t % 2, (t + 1) % 2
        each_side(has_lev, lambda side: lev_arrival(now, side).wait_recv())
        each_side(has_lon, lambda side: lon_arrival(now, side).wait_recv())
        if t >= 1:
            each_side(has_lev, lambda side: lev_copy(later, side).wait_send())
            each_side(has_lon, lambda side: lon_copy(later, side, t == 1).wait_send())

        def one_piece(c, carry):
            each_side(has_lat, lambda side: lat_arrival(now, side, c).wait_recv())
            if t >= 1:
                each_side(has_lat, lambda side: lat_copy(later, side, c, t == 1).wait_send())

            def one_column(i, carry):
                x = c * piece + i
                for y in range(rows):
                    value = advance(now, y, x)
                    cells[later, y + 1, x + 1] = value
                    lev_out[later, 0, y, x] = value[0:1, :]
                    lev_out[later, 1, y, x] = value[depth - 1 : depth, :]
                return carry

            lax.fori_loop(0, piece, one_column, 0)
            each_side(has_lat, lambda side: lat_copy(later, side, c).start())
            return carry

        lax.fori_loop(0, pieces, one_piece, 0)
        each_side(has_lev, lambda side: lev_copy(later, side).start())
        each_side(has_lon, lambda side: lon_copy(later, side).start())

    now, later = (STEPS - 1) % 2, STEPS % 2
    each_side(has_lev, lambda side: lev_arrival(now, side).wait_recv())
    each_side(has_lon, lambda side: lon_arrival(now, side).wait_recv())

    def last_columns(y, start, count):
        def one_column(i, carry):
            out_ref[y, start + i] = advance(now, y, start + i)
            return carry

        lax.fori_loop(0, count, one_column, 0)

    def stat_copy(y, k):
        return pltpu.make_async_remote_copy(
            src_ref=stat_in.at[0, y],
            dst_ref=stat_in.at[k, y],
            send_sem=stat_send.at[y, k],
            recv_sem=stat_recv.at[y, k],
            device_id={"lon": lax.rem(lon + k, lons)},
            device_id_type=MESH,
        )

    def send_stats(y):
        zero = jnp.zeros((depth, members), jnp.float32)
        mean = lax.fori_loop(0, width, lambda x, s: s + out_ref[y, x], zero) / width

        def square(x, s):
            d = out_ref[y, x] - mean
            return s + d * d

        stat_in[0, y, 0] = mean
        stat_in[0, y, 1] = lax.fori_loop(0, width, square, zero)
        for k in range(1, lons):
            stat_copy(y, k).start()

    def take_stats(y):
        for k in range(1, lons):
            stat_copy(y, k).wait()
        means = [stat_in[k, y, 0] for k in range(lons)]
        mean = functools.reduce(jnp.add, means) / lons
        squares = functools.reduce(jnp.add, [stat_in[k, y, 1] for k in range(lons)])
        apart = functools.reduce(jnp.add, [(m - mean) * (m - mean) for m in means])
        variance = squares / (width * lons) + apart / lons
        stat_ref[y, 0] = mean
        stat_ref[y, 1] = lax.rsqrt(variance + EPS)

    low = has_lat[0].astype(jnp.int32)
    high = rows - has_lat[1].astype(jnp.int32)

    def free_row(y, carry):
        last_columns(y, 0, width)
        send_stats(y)
        return carry

    lax.fori_loop(low, high, free_row, 0)

    def last_piece(c, carry):
        def finish(side):
            lat_arrival(now, side, c).wait_recv()
            lat_copy(later, side, c).wait_send()
            last_columns(0 if side == 0 else rows - 1, c * piece, piece)

        each_side(has_lat, finish)
        return carry

    lax.fori_loop(0, pieces, last_piece, 0)
    each_side(has_lat, lambda side: send_stats(0 if side == 0 else rows - 1))

    def take(y, carry):
        take_stats(y)
        return carry

    lax.fori_loop(low, high, take, 0)
    each_side(has_lat, lambda side: take_stats(0 if side == 0 else rows - 1))

    for parity in (0, 1):
        each_side(has_lev, lambda side: lev_copy(parity, side).wait_send())
        each_side(has_lon, lambda side: lon_copy(parity, side).wait_send())

    def drain(c, carry):
        each_side(has_lat, lambda side: lat_copy(now, side, c).wait_send())
        return carry

    lax.fori_loop(0, pieces, drain, 0)


def finish_kernel(state_ref, stat_ref, norm_hbm, temp_hbm, staged, norm_sem, temp_sem):
    rows, width = state_ref.shape[:2]
    temp = pltpu.make_async_copy(state_ref, temp_hbm, temp_sem)
    temp.start()
    for y in range(rows):
        mean, scale = stat_ref[y, 0], stat_ref[y, 1]

        def one_column(x, carry):
            staged[y, x] = (state_ref[y, x] - mean) * scale
            return carry

        lax.fori_loop(0, width, one_column, 0, unroll=4)
        pltpu.make_async_copy(staged.at[y], norm_hbm.at[y], norm_sem.at[y]).start()
    for y in range(rows):
        pltpu.make_async_copy(staged.at[y], norm_hbm.at[y], norm_sem.at[y]).wait()
    temp.wait()


def solution(mesh):
    lons = mesh.shape["lon"]

    def shards(initial_state, scaled_wind_north, scaled_wind_east, scaled_wind_upward):
        rows, width, depth, members = initial_state.shape
        pieces = pieces_of(width)
        f32 = jnp.float32
        dma = pltpu.SemaphoreType.DMA
        anywhere = pl.BlockSpec(memory_space=pl.ANY)
        inside = pl.BlockSpec(memory_space=pltpu.VMEM)
        state, stats = pl.pallas_call(
            functools.partial(march_kernel, pieces),
            out_shape=(
                pltpu.VMEM((rows, width, depth, members), f32),
                pltpu.VMEM((rows, 2, depth, members), f32),
            ),
            in_specs=[anywhere] * 4,
            out_specs=(inside, inside),
            scratch_shapes=[
                pltpu.VMEM((2, rows + 2, width + 2, depth, members), f32),
                pltpu.VMEM((3, rows, width, depth, members), f32),
                pltpu.VMEM((2, 2, rows, width, 1, members), f32),
                pltpu.VMEM((2, 2, rows, width, 1, members), f32),
                pltpu.VMEM((lons, rows, 2, depth, members), f32),
                dma((4,)),
                dma((2, 2, pieces)),
                dma((2, 2, pieces)),
                dma((2, 2)),
                dma((2, 2)),
                dma((2, 2)),
                dma((2, 2)),
                dma((rows, lons)),
                dma((rows, lons)),
            ],
            compiler_params=pltpu.CompilerParams(
                collective_id=0, has_side_effects=True, vmem_limit_bytes=44 * MIB
            ),
            name="march",
        )(initial_state, scaled_wind_north, scaled_wind_east, scaled_wind_upward)
        return pl.pallas_call(
            finish_kernel,
            out_shape=(jax.ShapeDtypeStruct((rows, width, depth, members), f32),) * 2,
            in_specs=[inside, inside],
            out_specs=(anywhere, anywhere),
            scratch_shapes=[
                pltpu.VMEM((rows, width, depth, members), f32),
                dma((rows,)),
                dma,
            ],
            compiler_params=pltpu.CompilerParams(vmem_limit_bytes=16 * MIB),
            name="finish",
        )(state, stats)

    spec = P("lat", "lon", "lev", None)
    return jax.shard_map(
        shards,
        mesh=mesh,
        in_specs=(spec,) * 4,
        out_specs=(spec, spec),
        check_vma=False,
    )
```

```python
import functools

import jax
import jax.numpy as jnp
from jax import lax
from jax.experimental import pallas as pl
from jax.experimental.pallas import tpu as pltpu
from jax.sharding import PartitionSpec as P

STEPS = 4
RATE = 0.05
EPS = 0.0001
MESH = pl.DeviceIdType.MESH
MIB = 1024 * 1024


def pieces_of(cells):
    return max(d for d in range(1, 9) if cells % d == 0)


def march_kernel(
    pieces, state_hbm, north_hbm, east_hbm, up_hbm, out_ref, stat_ref,
    cells, winds, lev_out, lev_in, stat_in, sums,
    load_sem, lat_send, lat_recv, tile_send, tile_recv,
    lon_send, lon_recv, lev_send, lev_recv, stat_send, stat_recv,
):
    rows, width, depth, members = out_ref.shape
    tiles, tile = stat_in.shape[2], stat_in.shape[4]
    piece = width // pieces
    head = max(pieces - 2, 0)
    lat, lon, lev = lax.axis_index("lat"), lax.axis_index("lon"), lax.axis_index("lev")
    lats, lons, levs = lax.axis_size("lat"), lax.axis_size("lon"), lax.axis_size("lev")
    has_lat = (lat > 0, lat < lats - 1)
    has_lon = (lon > 0, lon < lons - 1)
    has_lev = (lev > 0, lev < levs - 1)
    lat_peer = (jnp.maximum(lat - 1, 0), jnp.minimum(lat + 1, lats - 1))
    lon_peer = (jnp.maximum(lon - 1, 0), jnp.minimum(lon + 1, lons - 1))
    lev_peer = (jnp.maximum(lev - 1, 0), jnp.minimum(lev + 1, levs - 1))

    loads = [
        pltpu.make_async_copy(
            state_hbm, cells.at[0, pl.ds(1, rows), pl.ds(1, width)], load_sem.at[0]
        )
    ]
    for k, ref in enumerate((north_hbm, east_hbm, up_hbm)):
        loads.append(pltpu.make_async_copy(ref, winds.at[k], load_sem.at[k + 1]))
    loads[0].start()

    barrier = pltpu.get_barrier_semaphore()
    arrivals = lons - 1
    for axis, has, peer in (("lat", has_lat, lat_peer), ("lev", has_lev, lev_peer)):
        for side in (0, 1):
            arrivals = arrivals + has[side].astype(jnp.int32)

            @pl.when(has[side])
            def _(axis=axis, target=peer[side]):
                pl.semaphore_signal(barrier, inc=1, device_id={axis: target}, device_id_type=MESH)

    for k in range(1, lons):
        pl.semaphore_signal(
            barrier, inc=1, device_id={"lon": lax.rem(lon + k, lons)}, device_id_type=MESH
        )
    pl.semaphore_wait(barrier, arrivals)

    def lat_copy(parity, side, c, from_hbm=False):
        span = pl.ds(c * piece, piece)
        padded = pl.ds(1 + c * piece, piece)
        row = 0 if side == 0 else rows - 1
        src = state_hbm.at[row, span] if from_hbm else cells.at[parity, row + 1, padded]
        return pltpu.make_async_remote_copy(
            src_ref=src,
            dst_ref=cells.at[parity, rows + 1 if side == 0 else 0, padded],
            send_sem=lat_send.at[parity, side, c],
            recv_sem=lat_recv.at[parity, 1 - side, c],
            device_id={"lat": lat_peer[side]},
            device_id_type=MESH,
        )

    def lat_arrival(parity, side, c):
        here = cells.at[parity, 0 if side == 0 else rows + 1, pl.ds(1 + c * piece, piece)]
        return pltpu.make_async_remote_copy(
            src_ref=here, dst_ref=here,
            send_sem=lat_send.at[parity, side, c], recv_sem=lat_recv.at[parity, side, c],
            device_id={"lat": lat_peer[side]}, device_id_type=MESH,
        )

    def tile_copy(parity, side, k):
        span = pl.ds(1 + head * piece, width - head * piece)
        levels = pl.ds(k * tile, tile)
        return pltpu.make_async_remote_copy(
            src_ref=cells.at[parity, 1 if side == 0 else rows, span, levels],
            dst_ref=cells.at[parity, rows + 1 if side == 0 else 0, span, levels],
            send_sem=tile_send.at[side, k],
            recv_sem=tile_recv.at[1 - side, k],
            device_id={"lat": lat_peer[side]},
            device_id_type=MESH,
        )

    def tile_arrival(parity, side, k):
        span = pl.ds(1 + head * piece, width - head * piece)
        here = cells.at[parity, 0 if side == 0 else rows + 1, span, pl.ds(k * tile, tile)]
        return pltpu.make_async_remote_copy(
            src_ref=here, dst_ref=here,
            send_sem=tile_send.at[side, k], recv_sem=tile_recv.at[side, k],
            device_id={"lat": lat_peer[side]}, device_id_type=MESH,
        )

    def lon_copy(parity, side, from_hbm=False):
        col = 0 if side == 0 else width - 1
        mine = pl.ds(1, rows)
        src = state_hbm.at[:, col] if from_hbm else cells.at[parity, mine, col + 1]
        return pltpu.make_async_remote_copy(
            src_ref=src,
            dst_ref=cells.at[parity, mine, width + 1 if side == 0 else 0],
            send_sem=lon_send.at[parity, side],
            recv_sem=lon_recv.at[parity, 1 - side],
            device_id={"lon": lon_peer[side]},
            device_id_type=MESH,
        )

    def lon_arrival(parity, side):
        here = cells.at[parity, pl.ds(1, rows), 0 if side == 0 else width + 1]
        return pltpu.make_async_remote_copy(
            src_ref=here, dst_ref=here,
            send_sem=lon_send.at[parity, side], recv_sem=lon_recv.at[parity, side],
            device_id={"lon": lon_peer[side]}, device_id_type=MESH,
        )

    def lev_copy(parity, side):
        return pltpu.make_async_remote_copy(
            src_ref=lev_out.at[parity, side],
            dst_ref=lev_in.at[parity, 1 - side],
            send_sem=lev_send.at[parity, side],
            recv_sem=lev_recv.at[parity, 1 - side],
            device_id={"lev": lev_peer[side]},
            device_id_type=MESH,
        )

    def lev_arrival(parity, side):
        here = lev_in.at[parity, side]
        return pltpu.make_async_remote_copy(
            src_ref=here, dst_ref=here,
            send_sem=lev_send.at[parity, side], recv_sem=lev_recv.at[parity, side],
            device_id={"lev": lev_peer[side]}, device_id_type=MESH,
        )

    def each_side(has, act):
        for side in (0, 1):
            @pl.when(has[side])
            def _(side=side):
                act(side)

    def first_sends(c, carry):
        each_side(has_lat, lambda side: lat_copy(0, side, c, True).start())
        return carry

    lax.fori_loop(0, pieces, first_sends, 0)
    each_side(has_lon, lambda side: lon_copy(0, side, True).start())
    for load in loads[1:]:
        load.start()

    for side in (0, 1):
        @pl.when(jnp.logical_not(has_lat[side]))
        def _(row=0 if side == 0 else rows + 1):
            def clear(x, carry):
                for parity in (0, 1):
                    cells[parity, row, x + 1] = jnp.zeros((depth, members), jnp.float32)
                return carry

            lax.fori_loop(0, width, clear, 0)

        @pl.when(jnp.logical_not(has_lon[side]))
        def _(col=0 if side == 0 else width + 1):
            for parity in (0, 1):
                for y in range(rows):
                    cells[parity, y + 1, col] = jnp.zeros((depth, members), jnp.float32)

        @pl.when(jnp.logical_not(has_lev[side]))
        def _(side=side):
            def clear(x, carry):
                for parity in (0, 1):
                    for y in range(rows):
                        lev_in[parity, side, y, x] = jnp.zeros((1, members), jnp.float32)
                return carry

            lax.fori_loop(0, width, clear, 0)

    loads[0].wait()

    def first_levels(x, carry):
        for y in range(rows):
            lev_out[0, 0, y, x] = cells[0, y + 1, x + 1, 0:1, :]
            lev_out[0, 1, y, x] = cells[0, y + 1, x + 1, depth - 1 : depth, :]
        return carry

    lax.fori_loop(0, width, first_levels, 0)
    each_side(has_lev, lambda side: lev_copy(0, side).start())
    for load in loads[1:]:
        load.wait()

    level = lax.broadcasted_iota(jnp.int32, (depth, members), 0)
    bottom, top = level == 0, level == depth - 1

    def advance(parity, y, x, z=slice(None)):
        whole = cells[parity, y + 1, x + 1]
        mid = whole[z]
        south, north = cells[parity, y, x + 1, z], cells[parity, y + 2, x + 1, z]
        west, east = cells[parity, y + 1, x, z], cells[parity, y + 1, x + 2, z]
        below = jnp.where(bottom, lev_in[parity, 0, y, x], pltpu.roll(whole, 1, 0))[z]
        above = jnp.where(top, lev_in[parity, 1, y, x], pltpu.roll(whole, depth - 1, 0))[z]
        spread = (south + north) + (west + east) + (below + above) - 6.0 * mid
        return (
            mid
            - winds[0, y, x, z] * (north - south)
            - winds[1, y, x, z] * (east - west)
            - winds[2, y, x, z] * (above - below)
            + RATE * spread
        )

    for t in range(STEPS - 1):
        now, later = t % 2, (t + 1) % 2
        whole_pieces = head if t == STEPS - 2 else pieces
        each_side(has_lev, lambda side: lev_arrival(now, side).wait_recv())
        each_side(has_lon, lambda side: lon_arrival(now, side).wait_recv())
        if t >= 1:
            each_side(has_lev, lambda side: lev_copy(later, side).wait_send())
            each_side(has_lon, lambda side: lon_copy(later, side, t == 1).wait_send())

        def one_piece(c, carry):
            each_side(has_lat, lambda side: lat_arrival(now, side, c).wait_recv())
            if t >= 1:
                each_side(has_lat, lambda side: lat_copy(later, side, c, t == 1).wait_send())

            def one_column(i, carry):
                x = c * piece + i
                for y in range(rows):
                    value = advance(now, y, x)
                    cells[later, y + 1, x + 1] = value
                    lev_out[later, 0, y, x] = value[0:1, :]
                    lev_out[later, 1, y, x] = value[depth - 1 : depth, :]
                return carry

            lax.fori_loop(0, piece, one_column, 0)
            @pl.when(c < whole_pieces)
            def _():
                each_side(has_lat, lambda side: lat_copy(later, side, c).start())

            return carry

        lax.fori_loop(0, pieces, one_piece, 0)
        if t == STEPS - 2:
            for k in range(tiles):
                each_side(has_lat, lambda side: tile_copy(later, side, k).start())
        each_side(has_lev, lambda side: lev_copy(later, side).start())
        each_side(has_lon, lambda side: lon_copy(later, side).start())

    now, later = (STEPS - 1) % 2, STEPS % 2
    each_side(has_lev, lambda side: lev_arrival(now, side).wait_recv())
    each_side(has_lon, lambda side: lon_arrival(now, side).wait_recv())

    def open_row(y):
        sums[y, 0] = advance(now, y, 0)
        sums[y, 1] = jnp.zeros((depth, members), jnp.float32)
        sums[y, 2] = jnp.zeros((depth, members), jnp.float32)

    def last_columns(y, start, count, z=slice(None)):
        shift = sums[y, 0, z]

        def one_column(i, carry):
            total, square = carry
            value = advance(now, y, start + i, z)
            out_ref[y, start + i, z] = value
            moved = value - shift
            return total + moved, square + moved * moved

        total, square = lax.fori_loop(0, count, one_column, (sums[y, 1, z], sums[y, 2, z]))
        sums[y, 1, z] = total
        sums[y, 2, z] = square

    def levels_of(k):
        return slice(k * tile, (k + 1) * tile)

    def stat_copy(y, k, hop):
        return pltpu.make_async_remote_copy(
            src_ref=stat_in.at[0, y, k],
            dst_ref=stat_in.at[hop, y, k],
            send_sem=stat_send.at[y, k, hop],
            recv_sem=stat_recv.at[y, k, hop],
            device_id={"lon": lax.rem(lon + hop, lons)},
            device_id_type=MESH,
        )

    def send_stats(y, k):
        z = levels_of(k)
        total = sums[y, 1, z]
        stat_in[0, y, k, 0] = sums[y, 0, z] + total / width
        stat_in[0, y, k, 1] = jnp.maximum(sums[y, 2, z] - total * (total / width), 0.0)
        for hop in range(1, lons):
            stat_copy(y, k, hop).start()

    def take_stats(y, k):
        z = levels_of(k)
        for hop in range(1, lons):
            stat_copy(y, k, hop).wait()
        means = [stat_in[hop, y, k, 0] for hop in range(lons)]
        mean = functools.reduce(jnp.add, means) / lons
        squares = functools.reduce(jnp.add, [stat_in[hop, y, k, 1] for hop in range(lons)])
        apart = functools.reduce(jnp.add, [(m - mean) * (m - mean) for m in means])
        variance = squares / (width * lons) + apart / lons
        stat_ref[y, 0, z] = mean
        stat_ref[y, 1, z] = lax.rsqrt(variance + EPS)

    def edge_row(side):
        return 0 if side == 0 else rows - 1

    low = has_lat[0].astype(jnp.int32)
    high = rows - has_lat[1].astype(jnp.int32)

    def free_row(y, carry):
        open_row(y)
        last_columns(y, 0, width)
        for k in range(tiles):
            send_stats(y, k)
        return carry

    lax.fori_loop(low, high, free_row, 0)

    def sent_before(c, carry):
        each_side(has_lat, lambda side: lat_copy(later, side, c).wait_send())
        return carry

    def last_piece(c, carry):
        def finish(side):
            lat_arrival(now, side, c).wait_recv()

            @pl.when(c == 0)
            def _():
                open_row(edge_row(side))

            last_columns(edge_row(side), c * piece, piece)

        each_side(has_lat, finish)
        return carry

    lax.fori_loop(0, head, last_piece, 0)

    def take(y, carry):
        for k in range(tiles):
            take_stats(y, k)
        return carry

    lax.fori_loop(low, high, take, 0)
    lax.fori_loop(0, pieces, sent_before, 0)
    for k in range(tiles):
        def finish_tile(side):
            tile_arrival(now, side, k).wait_recv()
            last_columns(edge_row(side), head * piece, width - head * piece, levels_of(k))
            send_stats(edge_row(side), k)

        each_side(has_lat, finish_tile)
    for k in range(tiles):
        each_side(has_lat, lambda side: take_stats(edge_row(side), k))

    for parity in (0, 1):
        each_side(has_lev, lambda side: lev_copy(parity, side).wait_send())
        each_side(has_lon, lambda side: lon_copy(parity, side).wait_send())

    def drain(c, carry):
        each_side(has_lat, lambda side: lat_copy(now, side, c).wait_send())
        return carry

    lax.fori_loop(0, head, drain, 0)
    for k in range(tiles):
        each_side(has_lat, lambda side: tile_copy(now, side, k).wait_send())


def finish_kernel(state_ref, stat_ref, norm_hbm, temp_hbm, staged, norm_sem, temp_sem):
    rows, width = state_ref.shape[:2]
    temp = pltpu.make_async_copy(state_ref, temp_hbm, temp_sem)
    temp.start()
    for y in range(rows):
        mean, scale = stat_ref[y, 0], stat_ref[y, 1]

        def one_column(x, carry):
            staged[y, x] = (state_ref[y, x] - mean) * scale
            return carry

        lax.fori_loop(0, width, one_column, 0, unroll=4)
        pltpu.make_async_copy(staged.at[y], norm_hbm.at[y], norm_sem.at[y]).start()
    for y in range(rows):
        pltpu.make_async_copy(staged.at[y], norm_hbm.at[y], norm_sem.at[y]).wait()
    temp.wait()


def solution(mesh):
    lons = mesh.shape["lon"]

    def shards(initial_state, scaled_wind_north, scaled_wind_east, scaled_wind_upward):
        rows, width, depth, members = initial_state.shape
        pieces = pieces_of(width)
        tiles = depth // 8 if depth % 8 == 0 else 1
        f32 = jnp.float32
        dma = pltpu.SemaphoreType.DMA
        anywhere = pl.BlockSpec(memory_space=pl.ANY)
        inside = pl.BlockSpec(memory_space=pltpu.VMEM)
        state, stats = pl.pallas_call(
            functools.partial(march_kernel, pieces),
            out_shape=(
                pltpu.VMEM((rows, width, depth, members), f32),
                pltpu.VMEM((rows, 2, depth, members), f32),
            ),
            in_specs=[anywhere] * 4,
            out_specs=(inside, inside),
            scratch_shapes=[
                pltpu.VMEM((2, rows + 2, width + 2, depth, members), f32),
                pltpu.VMEM((3, rows, width, depth, members), f32),
                pltpu.VMEM((2, 2, rows, width, 1, members), f32),
                pltpu.VMEM((2, 2, rows, width, 1, members), f32),
                pltpu.VMEM((lons, rows, tiles, 2, depth // tiles, members), f32),
                pltpu.VMEM((rows, 3, depth, members), f32),
                dma((4,)),
                dma((2, 2, pieces)),
                dma((2, 2, pieces)),
                dma((2, tiles)),
                dma((2, tiles)),
                dma((2, 2)),
                dma((2, 2)),
                dma((2, 2)),
                dma((2, 2)),
                dma((rows, tiles, lons)),
                dma((rows, tiles, lons)),
            ],
            compiler_params=pltpu.CompilerParams(
                collective_id=0, has_side_effects=True, vmem_limit_bytes=44 * MIB
            ),
            name="march",
        )(initial_state, scaled_wind_north, scaled_wind_east, scaled_wind_upward)
        return pl.pallas_call(
            finish_kernel,
            out_shape=(jax.ShapeDtypeStruct((rows, width, depth, members), f32),) * 2,
            in_specs=[inside, inside],
            out_specs=(anywhere, anywhere),
            scratch_shapes=[
                pltpu.VMEM((rows, width, depth, members), f32),
                dma((rows,)),
                dma,
            ],
            compiler_params=pltpu.CompilerParams(vmem_limit_bytes=16 * MIB),
            name="finish",
        )(state, stats)

    spec = P("lat", "lon", "lev", None)
    return jax.shard_map(
        shards,
        mesh=mesh,
        in_specs=(spec,) * 4,
        out_specs=(spec, spec),
        check_vma=False,
    )
```
